32 devices in a mesh: row: 8 (over z, x), col: 4 (over y, core), ga: 1.
Axes of the slice: x: 2, y: 2, z: 4, core: 2. Of those that a mesh axis runs over, the one named last changes fastest.
Arguments:
- pair_density: float32 [512, 24, 3072], P('row', None, 'ga'), may hold values from -6 to 6
- coulomb: float32 [3072], P('ga'), may hold values from 0.1 to 2
Outputs:
- kernel: float32 [12288, 12288], P('row', 'col')
The draws below stay inside these ranges and needn't reach their ends.
All inputs are finite; a program needn't handle non-finite values.
Results may differ from the reference program's by a relative error of at most 0.00011.
Values sent between devices are 32-bit elements; how exact they have to be, the bound alone decides.
A program may use at most 192 MiB of HBM per device.

```python
import math
import jax
import jax.numpy as jnp
from jax import lax

NG = 3072
NK = 512
NVC = 24
N_ROW = 8
N_COL = 4


def level_of(own_key, extent, cuts, low, top_value):
    gain, own = 1.0, jax.random.fold_in(own_key, 6)
    for position, blocks in cuts:
        steps = jnp.exp(jax.random.uniform(jax.random.fold_in(own, position), (blocks,), jnp.float32, low / len(cuts), top_value / len(cuts)))
        gain = gain * jnp.repeat(steps, extent[position] // blocks).reshape([-1 if axis == position else 1 for axis in range(len(extent))])
    return gain


def bell_draw(rng, shape, spread, limit, split=(), kind=jnp.bfloat16):
    drawn = spread * jax.random.normal(rng, shape, jnp.float32)
    if split:
        drawn = drawn * level_of(rng, shape, split, -0.22, 0.18)
    return jnp.clip(drawn, -limit, limit).astype(kind)


def setup_inputs(seed: int = 0) -> dict:
    key_of = jax.random.split(jax.random.key(seed), 3)
    pair_density = bell_draw(key_of[0], (NK, NVC, NG), 1.0, 6.0, ((0, 8),), jnp.float32)
    coulomb = jnp.clip(jnp.exp(jax.random.uniform(key_of[1], (NG,), jnp.float32, math.log(0.1), math.log(2.0))), 0.1, 2.0)
    return {"pair_density": pair_density, "coulomb": coulomb}


def contract(left_rows, right_rows):
    return lax.dot_general(left_rows, right_rows, (((1,), (1,)), ((), ())), precision=lax.Precision.HIGHEST, preferred_element_type=jnp.float32)


def reference(pair_density, coulomb):
    row_order = jnp.arange(NK, dtype=jnp.int32).reshape(NK // N_ROW, N_ROW).T.reshape(-1)
    col_order = jnp.arange(NK, dtype=jnp.int32).reshape(NK // N_COL, N_COL).T.reshape(-1)
    left = pair_density[row_order]
    right = pair_density[col_order]
    bands = pair_density.shape[1]
    g_width = pair_density.shape[2]
    weighted = left.reshape(NK * bands, g_width) * (2.0 * coulomb)[None, :]
    exchange = contract(weighted, right.reshape(NK * bands, g_width))
    return exchange / jnp.float32(NK)
```

```python
import functools
import math

import jax
import jax.numpy as jnp
from jax import lax
from jax.experimental import pallas as pl
from jax.experimental.pallas import tpu as pltpu
from jax.sharding import PartitionSpec as P

MESH = pl.DeviceIdType.MESH
WIDTH = 256
FLIGHT = 4
SLOTS = FLIGHT + 2
TILE = 512


def ring_at(place, count):
    far = place // (count // 2)
    return (1 - far) * 2 * place + far * (2 * (count - 1 - place) + 1)


def place_of(row, count):
    odd = row % 2
    return (1 - odd) * (row // 2) + odd * (count - 1 - row // 2)


def flip(col, bit):
    return col + bit * (1 - 2 * ((col // bit) % 2))


def split(x):
    high = x.astype(jnp.bfloat16)
    return high, (x - high.astype(jnp.float32)).astype(jnp.bfloat16)


def kernel(
    sizes, pair_ref, scale_ref, out_ref, right, left, total, weighted, columns,
    own_sem, ring_send, ring_recv, left_send, left_recv, out_sem, ring_free, left_free,
):
    row_count, col_count, chunks, parts = sizes
    ratio = row_count // col_count
    per_class, bands = right.shape[2], right.shape[4]
    width = right.shape[5]
    here_row, here_col = lax.axis_index("row"), lax.axis_index("col")
    place = place_of(here_row, row_count)
    ahead = ring_at((place + 1) % row_count, row_count)
    behind = ring_at((place + row_count - 1) % row_count, row_count)
    home_col, home_class = here_row % col_count, here_row // col_count
    bits = [1 << b for b in range(int(math.log2(col_count)))]
    away = 0
    for bit in bits:
        away = away + bit * (((here_col // bit) + (home_col // bit)) % 2)
    period = row_count // FLIGHT
    group = row_count // parts

    def target(e):
        return ahead if e % 2 == 0 else behind

    def source_at(e, t):
        step = row_count - t if e % 2 == 0 else t
        return ring_at((place + step) % row_count, row_count)

    def own_copies(g):
        s = g % SLOTS
        cut = pl.ds(pl.multiple_of(g * width, width), width)
        return (
            pltpu.make_async_copy(
                pair_ref.at[:, :, here_col, :, cut], right.at[s, here_row], own_sem.at[s, 0]
            ),
            pltpu.make_async_copy(
                pair_ref.at[:, home_class, home_col, :, cut], left.at[s, here_row], own_sem.at[s, 1]
            ),
        )

    def ring_copy(s, t, e, q):
        return pltpu.make_async_remote_copy(
            src_ref=right.at[s, q, :, e],
            dst_ref=right.at[s, q, :, e],
            send_sem=ring_send.at[s, e],
            recv_sem=ring_recv.at[s, t, e],
            device_id={"row": target(e)},
            device_id_type=MESH,
        )

    def left_copy(src, s, t, q, b):
        return pltpu.make_async_remote_copy(
            src_ref=src,
            dst_ref=left.at[s, q],
            send_sem=left_send.at[s, b],
            recv_sem=left_recv.at[s, t],
            device_id={"col": flip(here_col, bits[b])},
            device_id_type=MESH,
        )

    def home_source(t):
        up = home_class % 2
        return (1 - up) * source_at(0, t) + up * source_at(1, t)

    def ring_event(g, t):
        s = g % SLOTS
        if t == 0:
            for copy in own_copies(g):
                copy.wait()

            @pl.when(g >= SLOTS)
            def _():
                for e in range(min(ratio, 2)):
                    pl.semaphore_wait(ring_free.at[e], 1)

            for e in range(ratio):
                ring_copy(s, 1, e, here_row).start()
            return
        for e in range(ratio):
            q = source_at(e, t)
            ring_copy(s, t, e, q).wait_recv()
            if t < row_count - 1:
                ring_copy(s, t + 1, e, q).start()
        q = home_source(t)

        @pl.when(away == 0)
        def _():
            for b in range(len(bits)):
                if t == 1:

                    @pl.when(g >= SLOTS)
                    def _():
                        pl.semaphore_wait(left_free.at[b], 1)

                left_copy(right.at[s, q, :, home_class], s, t, q, b).start()

        if t == 1:

            @pl.when(g + 1 < chunks)
            def _():
                for copy in own_copies(g + 1):
                    copy.start()

    def relay_event(g, t):
        s = g % SLOTS
        q = home_source(t)

        @pl.when((away > 0) & (away % 2 == 0))
        def _():
            left_copy(left.at[s, q], s, t, q, 0).wait_recv()
            for b, bit in enumerate(bits):

                @pl.when(away % (2 * bit) == 0)
                def _():
                    if t == 1:

                        @pl.when(g >= SLOTS)
                        def _():
                            pl.semaphore_wait(left_free.at[b], 1)

                    left_copy(left.at[s, q], s, t, q, b).start()

    def weigh(g):
        s = g % SLOTS
        rows = per_class * bands
        scale = scale_ref[g]

        @pl.when(away % 2 == 1)
        def _():
            for t in range(1, row_count):
                left_copy(left.at[s, 0], s, t, 0, 0).wait_recv()

        def fill(read):
            def one(q, _):
                high, low = split(read(q).reshape(rows, width) * scale)
                at = pl.ds(pl.multiple_of(q * rows, rows), rows)
                weighted[at, pl.ds(0, width)] = high
                weighted[at, pl.ds(width, width)] = high
                weighted[at, pl.ds(2 * width, width)] = low
                return 0

            lax.fori_loop(0, row_count, one, 0)

        @pl.when(away == 0)
        def _():
            fill(lambda q: right[s, q, :, home_class])

        @pl.when(away > 0)
        def _():
            fill(lambda q: left[s, q])

    def product(g, p):
        s = g % SLOTS
        block = group * per_class * ratio * bands
        high, low = split(right[s, pl.ds(p * group, group)].reshape(block, width))
        columns[:, pl.ds(0, width)] = high
        columns[:, pl.ds(width, width)] = low
        columns[:, pl.ds(2 * width, width)] = high
        tile = min(TILE, weighted.shape[0])

        def one(i, _):
            at = pl.ds(pl.multiple_of(i * tile, tile), tile)
            total[p, at, :] += lax.dot_general(
                weighted[at, :],
                columns[...],
                (((1,), (1,)), ((), ())),
                preferred_element_type=jnp.float32,
            )
            return 0

        lax.fori_loop(0, weighted.shape[0] // tile, one, 0)

        @pl.when(g == chunks - 1)
        def _():
            out_copy(p).start()

    def out_copy(p):
        block = total.shape[2]
        return pltpu.make_async_copy(
            total.at[p], out_ref.at[:, pl.ds(p * block, block)], out_sem.at[p]
        )

    def retire(g):
        s = g % SLOTS
        several = right.at[s, pl.ds(0, row_count - 1), :, 0]
        for e in range(ratio):
            pltpu.make_async_copy(several, several, ring_send.at[s, e]).wait()
        for b, bit in enumerate(bits):

            @pl.when(away % (2 * bit) == 0)
            def _():
                pltpu.make_async_copy(several, several, left_send.at[s, b]).wait()

        @pl.when(g + SLOTS < chunks)
        def _():
            for e in range(min(ratio, 2)):
                pl.semaphore_signal(
                    ring_free.at[e], inc=1, device_id={"row": behind if e == 0 else ahead}, device_id_type=MESH
                )
            for b, bit in enumerate(bits):

                @pl.when(away % (2 * bit) == bit)
                def _():
                    pl.semaphore_signal(
                        left_free.at[b], inc=1, device_id={"col": flip(here_col, bit)}, device_id_type=MESH
                    )

    for copy in own_copies(0):
        copy.start()
    barrier = pltpu.get_barrier_semaphore()
    for row in (ahead, behind):
        pl.semaphore_signal(barrier, inc=1, device_id={"row": row}, device_id_type=MESH)
    for bit in bits:
        pl.semaphore_signal(barrier, inc=1, device_id={"col": flip(here_col, bit)}, device_id_type=MESH)
    pl.semaphore_wait(barrier, 2 + len(bits))

    def clear(i, _):
        for p in range(parts):
            total[p, pl.ds(pl.multiple_of(i * 8, 8), 8), :] = jnp.zeros((8, total.shape[2]), jnp.float32)
        return 0

    lax.fori_loop(0, total.shape[1] // 8, clear, 0)

    def live(g, run):
        pl.when((g >= 0) & (g < chunks))(run)

    def round_of(base, _):
        for i in range(period):
            for d in range(FLIGHT + 1):
                t = i + d * period - 1
                if 1 <= t < row_count:
                    live(base - d, functools.partial(relay_event, base - d, t))
            for d in reversed(range(FLIGHT)):
                live(base - d, functools.partial(ring_event, base - d, i + d * period))
                if d % 2 == 0:
                    g = base - FLIGHT
                    p = 2 * i + (1 - d // 2)
                    if p == 0:
                        live(g, functools.partial(weigh, g))
                    if p < parts:
                        live(g, functools.partial(product, g, p))
        live(base - FLIGHT, functools.partial(retire, base - FLIGHT))
        return 0

    lax.fori_loop(0, chunks + FLIGHT, round_of, 0)
    for p in range(parts):
        out_copy(p).wait()


def local(pair_density, coulomb):
    row_count, col_count = lax.axis_size("row"), lax.axis_size("col")
    ratio = row_count // col_count
    local_k, bands, g_width = pair_density.shape
    total_k = local_k * row_count
    per_class = local_k // row_count
    width = math.gcd(WIDTH, g_width)
    chunks = g_width // width
    m, n = local_k * bands, total_k // col_count * bands
    piece = per_class * ratio * bands
    group = 1
    while group * piece % 256:
        group *= 2
    parts = row_count // group
    scale = ((2.0 * coulomb) / jnp.float32(total_k)).reshape(chunks, 1, width)
    pair = pair_density.reshape(per_class, ratio, col_count, bands, g_width)
    nbits = int(math.log2(col_count))
    f32 = jnp.float32
    total = pl.pallas_call(
        functools.partial(kernel, (row_count, col_count, chunks, parts)),
        out_shape=jax.ShapeDtypeStruct((m, n), f32),
        in_specs=[pl.BlockSpec(memory_space=pl.ANY), pl.BlockSpec(memory_space=pltpu.VMEM)],
        out_specs=pl.BlockSpec(memory_space=pl.ANY),
        scratch_shapes=[
            pltpu.VMEM((SLOTS, row_count, per_class, ratio, bands, width), f32),
            pltpu.VMEM((SLOTS, row_count, per_class, bands, width), f32),
            pltpu.VMEM((parts, m, group * piece), f32),
            pltpu.VMEM((m, 3 * width), jnp.bfloat16),
            pltpu.VMEM((group * piece, 3 * width), jnp.bfloat16),
            pltpu.SemaphoreType.DMA((SLOTS, 2)),
            pltpu.SemaphoreType.DMA((SLOTS, ratio)),
            pltpu.SemaphoreType.DMA((SLOTS, row_count, ratio)),
            pltpu.SemaphoreType.DMA((SLOTS, nbits)),
            pltpu.SemaphoreType.DMA((SLOTS, row_count)),
            pltpu.SemaphoreType.DMA((parts,)),
            pltpu.SemaphoreType.REGULAR((2,)),
            pltpu.SemaphoreType.REGULAR((nbits,)),
        ],
        compiler_params=pltpu.CompilerParams(
            collective_id=0, has_side_effects=True, vmem_limit_bytes=63 * 1024 * 1024
        ),
    )(pair, scale)
    return lax.psum(total, "ga")


def solution(mesh):
    placed = (P("row", None, "ga"), P("ga"))
    return jax.shard_map(
        local, mesh=mesh, in_specs=placed, out_specs=P("row", "col"), check_vma=False
    )
```

```python
import functools
import math

import jax
import jax.numpy as jnp
from jax import lax
from jax.experimental import pallas as pl
from jax.experimental.pallas import tpu as pltpu
from jax.sharding import PartitionSpec as P

MESH = pl.DeviceIdType.MESH
WIDTH = 256
FLIGHT = 2
SLOTS = FLIGHT + 3
HOLD = 36
TILE = 512
ROWS = 768
TAKE = 10


def ring_at(place, count):
    far = place // (count // 2)
    return (1 - far) * 2 * place + far * (2 * (count - 1 - place) + 1)


def place_of(row, count):
    odd = row % 2
    return (1 - odd) * (row // 2) + odd * (count - 1 - row // 2)


def flip(col, bit):
    return col + bit * (1 - 2 * ((col // bit) % 2))


def split(x):
    high = x.astype(jnp.bfloat16)
    return high, (x - high.astype(jnp.float32)).astype(jnp.bfloat16)


def contract(rows, columns):
    return lax.dot_general(
        rows, columns, (((1,), (1,)), ((), ())), preferred_element_type=jnp.float32
    )


def kernel(
    sizes, pair_ref, coulomb_ref, total, weighted, last, right, left, columns,
    own_sem, ring_send, ring_recv, left_send, left_recv, ring_free, left_free,
):
    row_count, col_count, chunks, parts, total_k = sizes
    ratio = row_count // col_count
    per_class, bands = right.shape[2], right.shape[4]
    width = right.shape[5]
    here_row, here_col = lax.axis_index("row"), lax.axis_index("col")
    place = place_of(here_row, row_count)
    ahead = ring_at((place + 1) % row_count, row_count)
    behind = ring_at((place + row_count - 1) % row_count, row_count)
    home_col, home_class = here_row % col_count, here_row // col_count
    bits = [1 << b for b in range(int(math.log2(col_count)))]
    away = 0
    for bit in bits:
        away = away + bit * (((here_col // bit) + (home_col // bit)) % 2)
    half = row_count // 2
    period = half // FLIGHT
    group = row_count // parts
    ways = (ahead, behind)

    def hops(way, e):
        return half if way == e % 2 else half - 1

    def source_at(way, t):
        return ring_at((place + (row_count - t if way == 0 else t)) % row_count, row_count)

    def own_copies(g):
        s = g % SLOTS
        cut = pl.ds(pl.multiple_of(g * width, width), width)
        return (
            pltpu.make_async_copy(
                pair_ref.at[:, :, here_col, :, cut], right.at[s, here_row], own_sem.at[s, 0]
            ),
            pltpu.make_async_copy(
                pair_ref.at[:, home_class, home_col, :, cut], left.at[s, here_row], own_sem.at[s, 1]
            ),
        )

    def ring_copy(s, way, e, q):
        return pltpu.make_async_remote_copy(
            src_ref=right.at[s, q, :, e],
            dst_ref=right.at[s, q, :, e],
            send_sem=ring_send.at[s, way, e],
            recv_sem=ring_recv.at[s, q, e],
            device_id={"row": ways[way]},
            device_id_type=MESH,
        )

    def left_copy(src, s, q, b):
        return pltpu.make_async_remote_copy(
            src_ref=src,
            dst_ref=left.at[s, q],
            send_sem=left_send.at[s, b],
            recv_sem=left_recv.at[s, q],
            device_id={"col": flip(here_col, bits[b])},
            device_id_type=MESH,
        )

    def ring_event(g, t):
        s = g % SLOTS
        if t == 0:
            for copy in own_copies(g):
                copy.wait()

            @pl.when(g >= SLOTS)
            def _():
                for way in range(2):
                    pl.semaphore_wait(ring_free.at[way], 1)

        for turn in range(2):
            for way in range(2):
                for e in range(ratio):
                    if (way + e) % 2 != turn or t > hops(way, e):
                        continue
                    q = here_row if t == 0 else source_at(way, t)
                    if t > 0:
                        ring_copy(s, way, e, q).wait_recv()
                    if t < hops(way, e):
                        ring_copy(s, way, e, q).start()
        if t == 0:
            return

        @pl.when(away == 0)
        def _():
            for b in range(len(bits)):
                if t == 1:

                    @pl.when(g >= SLOTS)
                    def _():
                        pl.semaphore_wait(left_free.at[b], 1)

                for way in range(1 if t == half else 2):
                    q = source_at(way, t)
                    left_copy(right.at[s, q, :, home_class], s, q, b).start()

        if t == 1:

            @pl.when(g + 1 < chunks)
            def _():
                for copy in own_copies(g + 1):
                    copy.start()

    def relay_event(g, t):
        s = g % SLOTS

        @pl.when((away > 0) & (away % 2 == 0))
        def _():
            for way in range(1 if t == half else 2):
                q = source_at(way, t)
                left_copy(left.at[s, q], s, q, 0).wait_recv()
                for b, bit in enumerate(bits):

                    @pl.when(away % (2 * bit) == 0)
                    def _():
                        if t == 1 and way == 0:

                            @pl.when(g >= SLOTS)
                            def _():
                                pl.semaphore_wait(left_free.at[b], 1)

                        left_copy(left.at[s, q], s, q, b).start()

    def weigh(g):
        s = g % SLOTS
        rows = per_class * bands

        def clear(i, _):
            for p in range(parts):
                total[p, pl.ds(pl.multiple_of(i * 8, 8), 8), :] = jnp.zeros((8, total.shape[2]), jnp.float32)
            return 0

        @pl.when(g == 0)
        def _():
            lax.fori_loop(0, total.shape[1] // 8, clear, 0)

        scale = (2.0 * coulomb_ref[g]) / jnp.float32(total_k)

        @pl.when(away % 2 == 1)
        def _():
            for t in range(1, half + 1):
                for way in range(1 if t == half else 2):
                    q = source_at(way, t)
                    left_copy(left.at[s, q], s, q, 0).wait_recv()

        def fill(read):
            def one(q, _):
                high, low = split(read(q).reshape(rows, width) * scale)
                at = pl.ds(pl.multiple_of(q * rows, rows), rows)
                weighted[at, pl.ds(0, width)] = high
                weighted[at, pl.ds(width, width)] = high
                weighted[at, pl.ds(2 * width, width)] = low
                return 0

            lax.fori_loop(0, row_count, one, 0)

        @pl.when(away == 0)
        def _():
            fill(lambda q: right[s, q, :, home_class])

        @pl.when(away > 0)
        def _():
            fill(lambda q: left[s, q])

    def product(g, p):
        s = g % SLOTS
        block = group * per_class * ratio * bands
        high, low = split(right[s, pl.ds(p * group, group)].reshape(block, width))

        @pl.when(g == chunks - 1)
        def _():
            last[p, :, pl.ds(0, width)] = high
            last[p, :, pl.ds(width, width)] = low
            last[p, :, pl.ds(2 * width, width)] = high

        @pl.when(g < chunks - 1)
        def _():
            columns[:, pl.ds(0, width)] = high
            columns[:, pl.ds(width, width)] = low
            columns[:, pl.ds(2 * width, width)] = high
            tile = min(TILE, weighted.shape[0])

            def one(i, _):
                at = pl.ds(pl.multiple_of(i * tile, tile), tile)
                total[p, at, :] += contract(weighted[at, :], columns[...])
                return 0

            lax.fori_loop(0, weighted.shape[0] // tile, one, 0)

    def retire(g):
        s = g % SLOTS
        for way in range(2):
            for e in range(ratio):
                several = right.at[s, pl.ds(0, hops(way, e)), :, e]
                pltpu.make_async_copy(several, several, ring_send.at[s, way, e]).wait()
        several = left.at[s, pl.ds(0, row_count - 1)]
        for b, bit in enumerate(bits):

            @pl.when(away % (2 * bit) == 0)
            def _():
                pltpu.make_async_copy(several, several, left_send.at[s, b]).wait()

        @pl.when(g + SLOTS < chunks)
        def _():
            for way in range(2):
                pl.semaphore_signal(
                    ring_free.at[way], inc=1, device_id={"row": ways[1 - way]}, device_id_type=MESH
                )
            for b, bit in enumerate(bits):

                @pl.when(away % (2 * bit) == bit)
                def _():
                    pl.semaphore_signal(
                        left_free.at[b], inc=1, device_id={"col": flip(here_col, bit)}, device_id_type=MESH
                    )

    for copy in own_copies(0):
        copy.start()
    barrier = pltpu.get_barrier_semaphore()
    for row in (ahead, behind):
        pl.semaphore_signal(barrier, inc=1, device_id={"row": row}, device_id_type=MESH)
    for bit in bits:
        pl.semaphore_signal(barrier, inc=1, device_id={"col": flip(here_col, bit)}, device_id_type=MESH)
    pl.semaphore_wait(barrier, 2 + len(bits))

    def live(g, run):
        pl.when((g >= 0) & (g < chunks))(run)

    turns = [(i, d) for i in range(period) for d in range(FLIGHT + 1) if 0 < i + d * period <= half]

    def round_of(base, _):
        done = base - FLIGHT - 1
        for i in range(period):
            for d in range(FLIGHT + 1):
                t = i + d * period
                if 2 <= t <= half + 1:
                    live(base - d, functools.partial(relay_event, base - d, t - 1))
                if t <= half:
                    live(base - d, functools.partial(ring_event, base - d, t))
                if (i, d) == turns[0]:
                    live(done, functools.partial(weigh, done))
                for p in range(parts):
                    if turns[p * len(turns) // parts] == (i, d):
                        live(done, functools.partial(product, done, p))
        live(done, functools.partial(retire, done))
        return 0

    lax.fori_loop(0, chunks + FLIGHT + 1, round_of, 0)


def finish(total, weighted, last, out_ref):
    p, i = pl.program_id(0), pl.program_id(1)
    rows = out_ref.shape[0]
    at = pl.ds(pl.multiple_of(i * rows, rows), rows)
    out_ref[...] = total[p, at, :] + contract(weighted[at, :], last[p])


def local(pair_density, coulomb):
    row_count, col_count = lax.axis_size("row"), lax.axis_size("col")
    ratio = row_count // col_count
    local_k, bands, g_width = pair_density.shape
    total_k = local_k * row_count
    per_class = local_k // row_count
    width = math.gcd(WIDTH, g_width)
    chunks = g_width // width
    m, n = local_k * bands, total_k // col_count * bands
    piece = per_class * ratio * bands
    group = 1
    while group * piece % 256:
        group *= 2
    parts = row_count // group
    coulomb = coulomb.reshape(chunks, 1, width)
    pair = pair_density.reshape(per_class, ratio, col_count, bands, g_width)
    nbits = int(math.log2(col_count))
    f32, block = jnp.float32, group * piece
    kept = [
        jax.ShapeDtypeStruct((parts, m, block), f32),
        jax.ShapeDtypeStruct((m, 3 * width), jnp.bfloat16),
        jax.ShapeDtypeStruct((parts, block, 3 * width), jnp.bfloat16),
    ]
    sums = pl.pallas_call(
        functools.partial(kernel, (row_count, col_count, chunks, parts, total_k)),
        out_shape=[pltpu.VMEM(x.shape, x.dtype) for x in kept],
        in_specs=[pl.BlockSpec(memory_space=pl.ANY), pl.BlockSpec(memory_space=pltpu.VMEM)],
        out_specs=[pl.BlockSpec(memory_space=pltpu.VMEM)] * 3,
        scratch_shapes=[
            pltpu.VMEM((SLOTS, row_count, per_class, ratio, bands, width), f32),
            pltpu.VMEM((SLOTS, row_count, per_class, bands, width), f32),
            pltpu.VMEM((block, 3 * width), jnp.bfloat16),
            pltpu.SemaphoreType.DMA((SLOTS, 2)),
            pltpu.SemaphoreType.DMA((SLOTS, 2, ratio)),
            pltpu.SemaphoreType.DMA((SLOTS, row_count, ratio)),
            pltpu.SemaphoreType.DMA((SLOTS, nbits)),
            pltpu.SemaphoreType.DMA((SLOTS, row_count)),
            pltpu.SemaphoreType.REGULAR((2,)),
            pltpu.SemaphoreType.REGULAR((nbits,)),
        ],
        compiler_params=pltpu.CompilerParams(
            collective_id=0, has_side_effects=True, vmem_limit_bytes=HOLD * 1024 * 1024
        ),
    )(pair, coulomb)
    rows = min(ROWS, m)
    total = pl.pallas_call(
        finish,
        grid=(parts, m // rows),
        out_shape=jax.ShapeDtypeStruct((m, n), f32),
        in_specs=[pl.BlockSpec(memory_space=pltpu.VMEM)] * 3,
        out_specs=pl.BlockSpec((rows, block), lambda p, i: (i, p)),
        compiler_params=pltpu.CompilerParams(vmem_limit_bytes=TAKE * 1024 * 1024),
    )(*sums)
    return lax.psum(total, "ga")


def solution(mesh):
    placed = (P("row", None, "ga"), P("ga"))
    return jax.shard_map(
        local, mesh=mesh, in_specs=placed, out_specs=P("row", "col"), check_vma=False
    )
```

```python
import functools
import math

import jax
import jax.numpy as jnp
from jax import lax
from jax.experimental import pallas as pl
from jax.experimental.pallas import tpu as pltpu
from jax.sharding import PartitionSpec as P

MESH = pl.DeviceIdType.MESH
WIDTH = 256
FLIGHT = 2
SLOTS = FLIGHT + 2
TILE = 512
ROWS = 768
HOLD, TAKE = 36, 10


def ring_at(place, count):
    far = place // (count // 2)
    return (1 - far) * 2 * place + far * (2 * (count - 1 - place) + 1)


def place_of(row, count):
    odd = row % 2
    return (1 - odd) * (row // 2) + odd * (count - 1 - row // 2)


def flip(col, bit):
    return col + bit * (1 - 2 * ((col // bit) % 2))


def split(x):
    high = x.astype(jnp.bfloat16)
    return high, (x - high.astype(jnp.float32)).astype(jnp.bfloat16)


def contract(rows, columns):
    return lax.dot_general(
        rows, columns, (((1,), (1,)), ((), ())), preferred_element_type=jnp.float32
    )


def kernel(
    sizes, pair_ref, coulomb_ref, total, weighted, last, right, left, columns,
    own_sem, ring_send, ring_recv, left_send, left_recv, ring_free, left_free,
):
    row_count, col_count, chunks, parts, total_k = sizes
    ratio = row_count // col_count
    per_class, bands = right.shape[2], right.shape[4]
    width = right.shape[5]
    here_row, here_col = lax.axis_index("row"), lax.axis_index("col")
    place = place_of(here_row, row_count)
    ahead = ring_at((place + 1) % row_count, row_count)
    behind = ring_at((place + row_count - 1) % row_count, row_count)
    home_col, home_class = here_row % col_count, here_row // col_count
    bits = [1 << b for b in range(int(math.log2(col_count)))]
    away = 0
    for bit in bits:
        away = away + bit * (((here_col // bit) + (home_col // bit)) % 2)
    half = row_count // 2
    period = half // FLIGHT
    group = row_count // parts
    ways = (ahead, behind)

    def hops(way, e):
        return half if way == e % 2 else half - 1

    def source_at(way, t):
        return ring_at((place + (row_count - t if way == 0 else t)) % row_count, row_count)

    def own_copies(g):
        s = g % SLOTS
        cut = pl.ds(pl.multiple_of(g * width, width), width)
        return (
            pltpu.make_async_copy(
                pair_ref.at[:, :, here_col, :, cut], right.at[s, here_row], own_sem.at[s, 0]
            ),
            pltpu.make_async_copy(
                pair_ref.at[:, home_class, home_col, :, cut], left.at[s, here_row], own_sem.at[s, 1]
            ),
        )

    def ring_copy(s, way, e, q):
        return pltpu.make_async_remote_copy(
            src_ref=right.at[s, q, :, e],
            dst_ref=right.at[s, q, :, e],
            send_sem=ring_send.at[s, way, e],
            recv_sem=ring_recv.at[s, q, e],
            device_id={"row": ways[way]},
            device_id_type=MESH,
        )

    def left_copy(src, s, q, b):
        return pltpu.make_async_remote_copy(
            src_ref=src,
            dst_ref=left.at[s, q],
            send_sem=left_send.at[s, b],
            recv_sem=left_recv.at[s, q],
            device_id={"col": flip(here_col, bits[b])},
            device_id_type=MESH,
        )

    def ring_event(g, t):
        s = g % SLOTS
        if t == 0:
            for copy in own_copies(g):
                copy.wait()

            @pl.when(g >= SLOTS)
            def _():
                for way in range(2):
                    pl.semaphore_wait(ring_free.at[way], 1)

        for turn in range(2):
            for way in range(2):
                for e in range(ratio):
                    if (way + e) % 2 != turn or t > hops(way, e):
                        continue
                    q = here_row if t == 0 else source_at(way, t)
                    if t > 0:
                        ring_copy(s, way, e, q).wait_recv()
                    if t < hops(way, e):
                        ring_copy(s, way, e, q).start()
        if t == 0:

            @pl.when(g + 1 < chunks)
            def _():
                for copy in own_copies(g + 1):
                    copy.start()

            return

        @pl.when(away == 0)
        def _():
            for b in range(len(bits)):
                if t == 1:

                    @pl.when(g >= SLOTS)
                    def _():
                        pl.semaphore_wait(left_free.at[b], 1)

                for way in range(1 if t == half else 2):
                    q = source_at(way, t)
                    left_copy(right.at[s, q, :, home_class], s, q, b).start()

    def relay_event(g, t):
        s = g % SLOTS

        @pl.when((away > 0) & (away % 2 == 0))
        def _():
            for way in range(1 if t == half else 2):
                q = source_at(way, t)
                left_copy(left.at[s, q], s, q, 0).wait_recv()
                for b, bit in enumerate(bits):

                    @pl.when(away % (2 * bit) == 0)
                    def _():
                        if t == 1 and way == 0:

                            @pl.when(g >= SLOTS)
                            def _():
                                pl.semaphore_wait(left_free.at[b], 1)

                        left_copy(left.at[s, q], s, q, b).start()

    def sources(steps):
        found = []
        for t in steps:
            if t == 0:
                found.append(here_row)
            for way in range(2 if 0 < t < half else t // half):
                found.append(source_at(way, t))
        return found

    def weigh(g, steps):
        s = g % SLOTS
        rows = per_class * bands
        scale = (2.0 * coulomb_ref[g]) / jnp.float32(total_k)

        @pl.when(away % 2 == 1)
        def _():
            for q in sources(t for t in steps if t):
                left_copy(left.at[s, q], s, q, 0).wait_recv()

        def fill(read):
            for q in sources(steps):
                high, low = split(read(q).reshape(rows, width) * scale)
                at = pl.ds(pl.multiple_of(q * rows, rows), rows)
                weighted[at, pl.ds(0, width)] = high
                weighted[at, pl.ds(width, width)] = high
                weighted[at, pl.ds(2 * width, width)] = low

        @pl.when(away == 0)
        def _():
            fill(lambda q: right[s, q, :, home_class])

        @pl.when(away > 0)
        def _():
            fill(lambda q: left[s, q])

    def clear():
        def one(i, _):
            for p in range(parts):
                total[p, pl.ds(pl.multiple_of(i * 8, 8), 8), :] = jnp.zeros((8, total.shape[2]), jnp.float32)
            return 0

        lax.fori_loop(0, total.shape[1] // 8, one, 0)

    def keep(g, steps):
        s = g % SLOTS
        piece = per_class * ratio * bands
        for q in sources(steps):
            high, low = split(right[s, q].reshape(piece, width))
            at = pl.ds(pl.multiple_of(q % group * piece, piece), piece)
            last[q // group, at, pl.ds(0, width)] = high
            last[q // group, at, pl.ds(width, width)] = low
            last[q // group, at, pl.ds(2 * width, width)] = high

    def prepare(g):
        weigh(g, range(half - 1))
        pl.when(g == 0)(clear)
        pl.when(g == chunks - 1)(functools.partial(keep, g, range(half)))

    def complete(g):
        weigh(g, range(half - 1, half + 1))
        pl.when(g == chunks - 1)(functools.partial(keep, g, range(half, half + 1)))

    def product(g, p):
        s = g % SLOTS
        block = group * per_class * ratio * bands

        @pl.when(g < chunks - 1)
        def _():
            high, low = split(right[s, pl.ds(p * group, group)].reshape(block, width))
            columns[:, pl.ds(0, width)] = high
            columns[:, pl.ds(width, width)] = low
            columns[:, pl.ds(2 * width, width)] = high
            tile = min(TILE, weighted.shape[0])

            def one(i, _):
                at = pl.ds(pl.multiple_of(i * tile, tile), tile)
                total[p, at, :] += contract(weighted[at, :], columns[...])
                return 0

            lax.fori_loop(0, weighted.shape[0] // tile, one, 0)

    def retire(g):
        s = g % SLOTS
        for way in range(2):
            for e in range(ratio):
                several = right.at[s, pl.ds(0, hops(way, e)), :, e]
                pltpu.make_async_copy(several, several, ring_send.at[s, way, e]).wait()
        several = left.at[s, pl.ds(0, row_count - 1)]
        for b, bit in enumerate(bits):

            @pl.when(away % (2 * bit) == 0)
            def _():
                pltpu.make_async_copy(several, several, left_send.at[s, b]).wait()

        @pl.when(g + SLOTS < chunks)
        def _():
            for way in range(2):
                pl.semaphore_signal(
                    ring_free.at[way], inc=1, device_id={"row": ways[1 - way]}, device_id_type=MESH
                )
            for b, bit in enumerate(bits):

                @pl.when(away % (2 * bit) == bit)
                def _():
                    pl.semaphore_signal(
                        left_free.at[b], inc=1, device_id={"col": flip(here_col, bit)}, device_id_type=MESH
                    )

    for copy in own_copies(0):
        copy.start()
    barrier = pltpu.get_barrier_semaphore()
    for row in (ahead, behind):
        pl.semaphore_signal(barrier, inc=1, device_id={"row": row}, device_id_type=MESH)
    for bit in bits:
        pl.semaphore_signal(barrier, inc=1, device_id={"col": flip(here_col, bit)}, device_id_type=MESH)
    pl.semaphore_wait(barrier, 2 + len(bits))

    def live(g, run):
        pl.when((g >= 0) & (g < chunks))(run)

    turns = [(i, d) for i in range(1, period) for d in range(FLIGHT)]

    def round_of(base, _):
        done = base - FLIGHT
        for i in range(period):
            for d in range(FLIGHT + 1):
                t = i + d * period
                if 2 <= t <= half + 1:
                    live(base - d, functools.partial(relay_event, base - d, t - 1))
            for d in range(FLIGHT + 1):
                t = i + d * period
                if t <= half:
                    live(base - d, functools.partial(ring_event, base - d, t))
                if (i, d) == turns[0]:
                    live(done, functools.partial(complete, done))
                for p in range(parts):
                    if turns[p * len(turns) // parts] == (i, d):
                        live(done, functools.partial(product, done, p))
        live(done, functools.partial(retire, done))
        live(done + 1, functools.partial(prepare, done + 1))
        return 0

    lax.fori_loop(0, chunks + FLIGHT, round_of, 0)


def finish(total, weighted, last, out_ref):
    p, i = pl.program_id(0), pl.program_id(1)
    rows = out_ref.shape[0]
    at = pl.ds(pl.multiple_of(i * rows, rows), rows)
    out_ref[...] = total[p, at, :] + contract(weighted[at, :], last[p])


def local(pair_density, coulomb):
    row_count, col_count = lax.axis_size("row"), lax.axis_size("col")
    ratio = row_count // col_count
    local_k, bands, g_width = pair_density.shape
    total_k = local_k * row_count
    per_class = local_k // row_count
    width = math.gcd(WIDTH, g_width)
    chunks = g_width // width
    m, n = local_k * bands, total_k // col_count * bands
    piece = per_class * ratio * bands
    group = 1
    while group * piece % 256:
        group *= 2
    parts = row_count // group
    coulomb = coulomb.reshape(chunks, 1, width)
    pair = pair_density.reshape(per_class, ratio, col_count, bands, g_width)
    nbits = int(math.log2(col_count))
    f32, block = jnp.float32, group * piece
    kept = [
        jax.ShapeDtypeStruct((parts, m, block), f32),
        jax.ShapeDtypeStruct((m, 3 * width), jnp.bfloat16),
        jax.ShapeDtypeStruct((parts, block, 3 * width), jnp.bfloat16),
    ]
    sums = pl.pallas_call(
        functools.partial(kernel, (row_count, col_count, chunks, parts, total_k)),
        out_shape=[pltpu.VMEM(x.shape, x.dtype) for x in kept],
        in_specs=[pl.BlockSpec(memory_space=pl.ANY), pl.BlockSpec(memory_space=pltpu.VMEM)],
        out_specs=[pl.BlockSpec(memory_space=pltpu.VMEM)] * 3,
        scratch_shapes=[
            pltpu.VMEM((SLOTS, row_count, per_class, ratio, bands, width), f32),
            pltpu.VMEM((SLOTS, row_count, per_class, bands, width), f32),
            pltpu.VMEM((block, 3 * width), jnp.bfloat16),
            pltpu.SemaphoreType.DMA((SLOTS, 2)),
            pltpu.SemaphoreType.DMA((SLOTS, 2, ratio)),
            pltpu.SemaphoreType.DMA((SLOTS, row_count, ratio)),
            pltpu.SemaphoreType.DMA((SLOTS, nbits)),
            pltpu.SemaphoreType.DMA((SLOTS, row_count)),
            pltpu.SemaphoreType.REGULAR((2,)),
            pltpu.SemaphoreType.REGULAR((nbits,)),
        ],
        compiler_params=pltpu.CompilerParams(
            collective_id=0, has_side_effects=True, vmem_limit_bytes=HOLD * 1024 * 1024
        ),
    )(pair, coulomb)
    rows = min(ROWS, m)
    total = pl.pallas_call(
        finish,
        grid=(parts, m // rows),
        out_shape=jax.ShapeDtypeStruct((m, n), f32),
        in_specs=[pl.BlockSpec(memory_space=pltpu.VMEM)] * 3,
        out_specs=pl.BlockSpec((rows, block), lambda p, i: (i, p)),
        compiler_params=pltpu.CompilerParams(vmem_limit_bytes=TAKE * 1024 * 1024),
    )(*sums)
    return lax.psum(total, "ga")


def solution(mesh):
    placed = (P("row", None, "ga"), P("ga"))
    return jax.shard_map(
        local, mesh=mesh, in_specs=placed, out_specs=P("row", "col"), check_vma=False
    )
```

```python
import functools
import math

import jax
import jax.numpy as jnp
from jax import lax
from jax.experimental import pallas as pl
from jax.experimental.pallas import tpu as pltpu
from jax.sharding import PartitionSpec as P

MESH = pl.DeviceIdType.MESH
WIDTH = 256
FLIGHT = 2
SLOTS = FLIGHT + 2
TILE = 768
ROWS = 768
HOLD, TAKE = 36, 10


def ring_at(place, count):
    far = place // (count // 2)
    return (1 - far) * 2 * place + far * (2 * (count - 1 - place) + 1)


def place_of(row, count):
    odd = row % 2
    return (1 - odd) * (row // 2) + odd * (count - 1 - row // 2)


def flip(col, bit):
    return col + bit * (1 - 2 * ((col // bit) % 2))


def split(x):
    high = x.astype(jnp.bfloat16)
    return high, (x - high.astype(jnp.float32)).astype(jnp.bfloat16)


def contract(rows, columns):
    return lax.dot_general(
        rows, columns, (((1,), (1,)), ((), ())), preferred_element_type=jnp.float32
    )


def kernel(
    sizes, pair_ref, coulomb_ref, total, weighted, last, right, left, columns,
    own_sem, ring_send, ring_recv, left_send, left_recv, ring_free, left_free,
):
    row_count, col_count, chunks, parts, total_k = sizes
    ratio = row_count // col_count
    per_class, bands = right.shape[2], right.shape[4]
    width = right.shape[5]
    here_row, here_col = lax.axis_index("row"), lax.axis_index("col")
    place = place_of(here_row, row_count)
    ahead = ring_at((place + 1) % row_count, row_count)
    behind = ring_at((place + row_count - 1) % row_count, row_count)
    home_col, home_class = here_row % col_count, here_row // col_count
    bits = [1 << b for b in range(int(math.log2(col_count)))]
    away = 0
    for bit in bits:
        away = away + bit * (((here_col // bit) + (home_col // bit)) % 2)
    half = row_count // 2
    period = half // FLIGHT
    group = row_count // parts
    ways = (ahead, behind)

    def hops(way, e):
        return half if way == e % 2 else half - 1

    def source_at(way, t):
        return ring_at((place + (row_count - t if way == 0 else t)) % row_count, row_count)

    def own_copies(g):
        s = g % SLOTS
        cut = pl.ds(pl.multiple_of(g * width, width), width)
        return (
            pltpu.make_async_copy(
                pair_ref.at[:, :, here_col, :, cut], right.at[s, here_row], own_sem.at[s, 0]
            ),
            pltpu.make_async_copy(
                pair_ref.at[:, home_class, home_col, :, cut], left.at[s, here_row], own_sem.at[s, 1]
            ),
        )

    def ring_copy(s, way, e, q):
        return pltpu.make_async_remote_copy(
            src_ref=right.at[s, q, :, e],
            dst_ref=right.at[s, q, :, e],
            send_sem=ring_send.at[s, way, e],
            recv_sem=ring_recv.at[s, q, e],
            device_id={"row": ways[way]},
            device_id_type=MESH,
        )

    def left_copy(src, s, q, b):
        return pltpu.make_async_remote_copy(
            src_ref=src,
            dst_ref=left.at[s, q],
            send_sem=left_send.at[s, b],
            recv_sem=left_recv.at[s, q],
            device_id={"col": flip(here_col, bits[b])},
            device_id_type=MESH,
        )

    def ring_event(g, t):
        s = g % SLOTS
        if t == 0:
            for copy in own_copies(g):
                copy.wait()

            @pl.when(g >= SLOTS)
            def _():
                for way in range(2):
                    pl.semaphore_wait(ring_free.at[way], 1)

        for turn in range(2):
            for way in range(2):
                for e in range(ratio):
                    if (way + e) % 2 != turn or t > hops(way, e):
                        continue
                    q = here_row if t == 0 else source_at(way, t)
                    if t > 0:
                        ring_copy(s, way, e, q).wait_recv()
                    if t < hops(way, e):
                        ring_copy(s, way, e, q).start()
        if t == 0:

            @pl.when(g + 1 < chunks)
            def _():
                for copy in own_copies(g + 1):
                    copy.start()

            return

        @pl.when(away == 0)
        def _():
            for b in range(len(bits)):
                if t == 1:

                    @pl.when(g >= SLOTS)
                    def _():
                        pl.semaphore_wait(left_free.at[b], 1)

                for way in range(1 if t == half else 2):
                    q = source_at(way, t)
                    left_copy(right.at[s, q, :, home_class], s, q, b).start()

    def relay_event(g, t):
        s = g % SLOTS

        @pl.when((away > 0) & (away % 2 == 0))
        def _():
            for way in range(1 if t == half else 2):
                q = source_at(way, t)
                left_copy(left.at[s, q], s, q, 0).wait_recv()
                for b, bit in enumerate(bits):

                    @pl.when(away % (2 * bit) == 0)
                    def _():
                        if t == 1 and way == 0:

                            @pl.when(g >= SLOTS)
                            def _():
                                pl.semaphore_wait(left_free.at[b], 1)

                        left_copy(left.at[s, q], s, q, b).start()

    def sources(steps):
        found = []
        for t in steps:
            if t == 0:
                found.append(here_row)
            for way in range(2 if 0 < t < half else t // half):
                found.append(source_at(way, t))
        return found

    def weigh(g, steps):
        s = g % SLOTS
        rows = per_class * bands
        scale = (2.0 * coulomb_ref[g]) / jnp.float32(total_k)

        @pl.when(away % 2 == 1)
        def _():
            for q in sources(t for t in steps if t):
                left_copy(left.at[s, q], s, q, 0).wait_recv()

        def fill(read):
            for q in sources(steps):
                high, low = split(read(q).reshape(rows, width) * scale)
                at = pl.ds(pl.multiple_of(q * rows, rows), rows)
                weighted[at, pl.ds(0, width)] = high
                weighted[at, pl.ds(width, width)] = high
                weighted[at, pl.ds(2 * width, width)] = low

        @pl.when(away == 0)
        def _():
            fill(lambda q: right[s, q, :, home_class])

        @pl.when(away > 0)
        def _():
            fill(lambda q: left[s, q])

    def clear():
        def one(i, _):
            for p in range(parts):
                total[p, pl.ds(pl.multiple_of(i * 8, 8), 8), :] = jnp.zeros((8, total.shape[2]), jnp.float32)
            return 0

        lax.fori_loop(0, total.shape[1] // 8, one, 0)

    def keep(g, steps):
        s = g % SLOTS
        piece = per_class * ratio * bands
        for q in sources(steps):
            high, low = split(right[s, q].reshape(piece, width))
            at = pl.ds(pl.multiple_of(q % group * piece, piece), piece)
            last[q // group, at, pl.ds(0, width)] = high
            last[q // group, at, pl.ds(width, width)] = low
            last[q // group, at, pl.ds(2 * width, width)] = high

    def prepare(g):
        weigh(g, range(half - 1))
        pl.when(g == 0)(clear)
        pl.when(g == chunks - 1)(functools.partial(keep, g, range(half)))

    def complete(g):
        pl.when(g == chunks - 1)(functools.partial(keep, g, range(half, half + 1)))
        weigh(g, range(half - 1, half))
        weigh(g, range(half, half + 1))

    def product(g, p):
        s = g % SLOTS
        block = group * per_class * ratio * bands

        @pl.when(g < chunks - 1)
        def _():
            high, low = split(right[s, pl.ds(p * group, group)].reshape(block, width))
            columns[:, pl.ds(0, width)] = high
            columns[:, pl.ds(width, width)] = low
            columns[:, pl.ds(2 * width, width)] = high
            tile = min(TILE, weighted.shape[0])

            def one(i, _):
                at = pl.ds(pl.multiple_of(i * tile, tile), tile)
                total[p, at, :] += contract(weighted[at, :], columns[...])
                return 0

            lax.fori_loop(0, weighted.shape[0] // tile, one, 0)

    def retire(g):
        s = g % SLOTS
        for way in range(2):
            for e in range(ratio):
                several = right.at[s, pl.ds(0, hops(way, e)), :, e]
                pltpu.make_async_copy(several, several, ring_send.at[s, way, e]).wait()
        several = left.at[s, pl.ds(0, row_count - 1)]
        for b, bit in enumerate(bits):

            @pl.when(away % (2 * bit) == 0)
            def _():
                pltpu.make_async_copy(several, several, left_send.at[s, b]).wait()

        @pl.when(g + SLOTS < chunks)
        def _():
            for way in range(2):
                pl.semaphore_signal(
                    ring_free.at[way], inc=1, device_id={"row": ways[1 - way]}, device_id_type=MESH
                )
            for b, bit in enumerate(bits):

                @pl.when(away % (2 * bit) == bit)
                def _():
                    pl.semaphore_signal(
                        left_free.at[b], inc=1, device_id={"col": flip(here_col, bit)}, device_id_type=MESH
                    )

    for copy in own_copies(0):
        copy.start()
    barrier = pltpu.get_barrier_semaphore()
    for row in (ahead, behind):
        pl.semaphore_signal(barrier, inc=1, device_id={"row": row}, device_id_type=MESH)
    for bit in bits:
        pl.semaphore_signal(barrier, inc=1, device_id={"col": flip(here_col, bit)}, device_id_type=MESH)
    pl.semaphore_wait(barrier, 2 + len(bits))

    def live(g, run):
        pl.when((g >= 0) & (g < chunks))(run)

    turns = [(i, d) for i in range(1, period) for d in range(FLIGHT)]

    def round_of(base, _):
        done = base - FLIGHT
        for i in range(period):
            for d in range(FLIGHT + 1):
                t = i + d * period
                if 2 <= t <= half + 1:
                    live(base - d, functools.partial(relay_event, base - d, t - 1))
            for d in range(FLIGHT + 1):
                t = i + d * period
                if t <= half:
                    live(base - d, functools.partial(ring_event, base - d, t))
                if (i, d) == turns[0]:
                    live(done, functools.partial(complete, done))
                for p in range(parts):
                    if turns[p * len(turns) // parts] == (i, d):
                        live(done, functools.partial(product, done, p))
        live(done, functools.partial(retire, done))
        live(done + 1, functools.partial(prepare, done + 1))
        return 0

    lax.fori_loop(0, chunks + FLIGHT, round_of, 0)


def finish(total, weighted, last, out_ref):
    p, i = pl.program_id(0), pl.program_id(1)
    rows = out_ref.shape[0]
    at = pl.ds(pl.multiple_of(i * rows, rows), rows)
    out_ref[...] = total[p, at, :] + contract(weighted[at, :], last[p])


def local(pair_density, coulomb):
    row_count, col_count = lax.axis_size("row"), lax.axis_size("col")
    ratio = row_count // col_count
    local_k, bands, g_width = pair_density.shape
    total_k = local_k * row_count
    per_class = local_k // row_count
    width = math.gcd(WIDTH, g_width)
    chunks = g_width // width
    m, n = local_k * bands, total_k // col_count * bands
    piece = per_class * ratio * bands
    group = 1
    while group * piece % 256:
        group *= 2
    parts = row_count // group
    coulomb = coulomb.reshape(chunks, 1, width)
    pair = pair_density.reshape(per_class, ratio, col_count, bands, g_width)
    nbits = int(math.log2(col_count))
    f32, block = jnp.float32, group * piece
    kept = [
        jax.ShapeDtypeStruct((parts, m, block), f32),
        jax.ShapeDtypeStruct((m, 3 * width), jnp.bfloat16),
        jax.ShapeDtypeStruct((parts, block, 3 * width), jnp.bfloat16),
    ]
    sums = pl.pallas_call(
        functools.partial(kernel, (row_count, col_count, chunks, parts, total_k)),
        out_shape=[pltpu.VMEM(x.shape, x.dtype) for x in kept],
        in_specs=[pl.BlockSpec(memory_space=pl.ANY), pl.BlockSpec(memory_space=pltpu.VMEM)],
        out_specs=[pl.BlockSpec(memory_space=pltpu.VMEM)] * 3,
        scratch_shapes=[
            pltpu.VMEM((SLOTS, row_count, per_class, ratio, bands, width), f32),
            pltpu.VMEM((SLOTS, row_count, per_class, bands, width), f32),
            pltpu.VMEM((block, 3 * width), jnp.bfloat16),
            pltpu.SemaphoreType.DMA((SLOTS, 2)),
            pltpu.SemaphoreType.DMA((SLOTS, 2, ratio)),
            pltpu.SemaphoreType.DMA((SLOTS, row_count, ratio)),
            pltpu.SemaphoreType.DMA((SLOTS, nbits)),
            pltpu.SemaphoreType.DMA((SLOTS, row_count)),
            pltpu.SemaphoreType.REGULAR((2,)),
            pltpu.SemaphoreType.REGULAR((nbits,)),
        ],
        compiler_params=pltpu.CompilerParams(
            collective_id=0, has_side_effects=True, vmem_limit_bytes=HOLD * 1024 * 1024
        ),
    )(pair, coulomb)
    rows = min(ROWS, m)
    total = pl.pallas_call(
        finish,
        grid=(parts, m // rows),
        out_shape=jax.ShapeDtypeStruct((m, n), f32),
        in_specs=[pl.BlockSpec(memory_space=pltpu.VMEM)] * 3,
        out_specs=pl.BlockSpec((rows, block), lambda p, i: (i, p)),
        compiler_params=pltpu.CompilerParams(vmem_limit_bytes=TAKE * 1024 * 1024),
    )(*sums)
    return lax.psum(total, "ga")


def solution(mesh):
    placed = (P("row", None, "ga"), P("ga"))
    return jax.shard_map(
        local, mesh=mesh, in_specs=placed, out_specs=P("row", "col"), check_vma=False
    )
```
